32 devices in a mesh: dp: 8 (over z, y), tensor: 4 (over x, core).
Axes of the slice: x: 2, y: 2, z: 4, core: 2. Of those that a mesh axis runs over, the one named last changes fastest.
Arguments:
- sampled_earlier_tokens: int32 [32, 169], P('dp'), may hold values from 0 to 4095
- quantizer_vectors: float32 [4096, 32], replicated, may hold values from -6 to 6
- summed_latent_canvas: float32 [32, 256, 32], P('dp'), may hold values from -6 to 6
- latent_lift_matrix: float32 [32, 1536], replicated, may hold values from -1 to 1
- location_tier_offset: float32 [256, 1536], replicated, may hold values from -3 to 3
- adaptive_norm_factors: float32 [1, 32, 6, 1536], P(None, 'dp'), may hold values from -3 to 3
- logit_sharpness: float32 [1, 16], P(None, 'tensor'), may hold values from 2 to 240, as said below
- probe_match_content_matrix: bfloat16 [1, 1536, 3, 1536], P(None, 'dp', None, 'tensor'), may hold values from -1 to 1, as said below
- mixing_projection_matrix: bfloat16 [1, 1536, 1536], P(None, 'tensor', 'dp'), may hold values from -0.15625 to 0.15625
- widening_projection_matrix: bfloat16 [1, 1536, 6144], P(None, 'dp', 'tensor'), may hold values from -0.15625 to 0.15625
- narrowing_projection_matrix: bfloat16 [1, 6144, 1536], P(None, 'tensor', 'dp'), may hold values from -0.078125 to 0.078125
- cached_lower_grid_lookups: bfloat16 [1, 32, 424, 1536], P(None, 'dp', None, 'tensor'), may hold values from -6 to 6
- cached_lower_grid_payloads: bfloat16 [1, 32, 424, 1536], P(None, 'dp', None, 'tensor'), may hold values from -6 to 6
- final_norm_factors: float32 [32, 2, 1536], P('dp'), may hold values from -3 to 3
- vocabulary_logit_matrix: bfloat16 [1536, 4096], P(None, 'tensor'), may hold values from -0.15625 to 0.15625
Outputs:
- logits: bfloat16 [32, 256, 4096], P('dp', None, 'tensor')
- canvas: float32 [32, 256, 32], P('dp')
The draws below stay inside these ranges and needn't reach their ends.
Inputs may be any that keep to these rules, and one draw needn't show every extreme that they name: `logit_sharpness`: Positive. `probe_match_content_matrix`: entries of spread about 1536 ** -0.5.
All inputs are finite; a program needn't handle non-finite values.
Results may differ from the reference program's by a relative error of at most 0.015.
Values may be sent and summed in bfloat16 or wider, within the bound.
A program may use at most 128 MiB of HBM per device.

```python
import math
import jax
import jax.numpy as jnp
from jax import lax

D = 1536
HEADS = 16
HDIM = 96
FF = 6144
VOCAB = 4096
CVAE = 32
LAYERS = 1
SIDE = 16
PREV = 13
CACHE = 424
TOK = 256
PREVTOK = 169
IMAGES = 32
N_TENSOR = 4


def draw_probe_match_content_matrix(key, part):
    base_draw = jax.random.truncated_normal(jax.random.fold_in(key, 11), -6.0, 6.0, (LAYERS, D, 3, D), jnp.float32) * D ** (-0.5)
    drawn_values = base_draw
    return drawn_values.astype(jnp.bfloat16)


def draw_logit_sharpness(key, part):
    exponent = jax.random.uniform(jax.random.fold_in(key, 23), (LAYERS, HEADS), jnp.float32, math.log(2.0), math.log(60.0))
    drawn_values = jnp.exp(exponent)
    return drawn_values


def plant(array, stream_key, least, top_value):
    extent = array.shape
    place = [jax.random.randint(jax.random.fold_in(stream_key, axis), (), 0, extent[axis]) for axis in range(len(extent))]
    array = array.at[tuple(place)].set(least)
    longest = extent.index(max(extent))
    place[longest] = (place[longest] + 1) % extent[longest]
    return array.at[tuple(place)].set(top_value)


def block_levels(key, dims, pieces, smallest, largest):
    factor_of = 1.0
    for dim, parts in pieces:
        draws = jax.random.uniform(jax.random.fold_in(jax.random.fold_in(key, 6), dim), (parts,), jnp.float32, smallest / len(pieces), largest / len(pieces))
        factor_of = factor_of * jnp.repeat(jnp.exp(draws), dims[dim] // parts).reshape((-1,) + (1,) * (len(dims) - 1 - dim))
    return factor_of


def noise(key, dims, width, bound, cuts=(), kind=jnp.bfloat16):
    array = jax.random.normal(key, dims, jnp.float32) * width
    if len(cuts) > 0:
        array = block_levels(key, dims, cuts, -0.22, 0.18) * array
    return jnp.clip(array, min=-bound, max=bound).astype(kind)


def setup_inputs(seed: int = 0) -> dict:
    streams_of = jax.random.split(jax.random.key(seed), 16)
    return {
        "sampled_earlier_tokens": plant(jax.random.randint(streams_of[0], (IMAGES, PREVTOK), 0, VOCAB), jax.random.fold_in(streams_of[0], 1), 0, VOCAB - 1).astype(jnp.int32),
        "quantizer_vectors": noise(streams_of[1], (VOCAB, CVAE), 1.0, 6.0, (), jnp.float32),
        "summed_latent_canvas": noise(streams_of[2], (IMAGES, TOK, CVAE), 1.0, 6.0, ((0, 8),), jnp.float32),
        "latent_lift_matrix": noise(streams_of[3], (CVAE, D), CVAE ** -0.5, 1.0, (), jnp.float32),
        "location_tier_offset": noise(streams_of[4], (TOK, D), 0.5, 3.0, (), jnp.float32),
        "adaptive_norm_factors": noise(streams_of[5], (LAYERS, IMAGES, 6, D), 0.5, 3.0, ((1, 8),), jnp.float32),
        "logit_sharpness": draw_logit_sharpness(jax.random.fold_in(streams_of[15], 71), 0),
        "probe_match_content_matrix": draw_probe_match_content_matrix(jax.random.fold_in(streams_of[15], 71), 0),
        "mixing_projection_matrix": noise(streams_of[8], (LAYERS, D, D), D ** -0.5, 0.15625, ((1, 4), (2, 8))),
        "widening_projection_matrix": noise(streams_of[9], (LAYERS, D, FF), D ** -0.5, 0.15625, ((1, 8), (2, 4))),
        "narrowing_projection_matrix": noise(streams_of[10], (LAYERS, FF, D), FF ** -0.5, 0.078125, ((1, 4), (2, 8))),
        "cached_lower_grid_lookups": noise(streams_of[11], (LAYERS, IMAGES, CACHE, D), 1.0, 6.0, ((1, 8), (3, 4))),
        "cached_lower_grid_payloads": noise(streams_of[12], (LAYERS, IMAGES, CACHE, D), 1.0, 6.0, ((1, 8), (3, 4))),
        "final_norm_factors": noise(streams_of[13], (IMAGES, 2, D), 0.5, 3.0, ((0, 8),), jnp.float32),
        "vocabulary_logit_matrix": noise(streams_of[14], (D, VOCAB), D ** -0.5, 0.15625, ((1, 4),)),
    }


norm_floor = 0.1
highest = lax.Precision.HIGHEST

def interp_matrix(grid_side, prev_side):
    out_cells = jnp.arange(grid_side, dtype=jnp.int32)
    numerator = jnp.maximum((2 * out_cells + 1) * prev_side - grid_side, 0)
    lower_cell = numerator // (2 * grid_side)
    fraction = (numerator % (2 * grid_side)).astype(jnp.float32) / (2.0 * grid_side)
    upper_cell = jnp.minimum(lower_cell + 1, prev_side - 1)
    in_cells = jnp.arange(prev_side, dtype=jnp.int32)
    lower_hit = (in_cells[None, :] == lower_cell[:, None]).astype(jnp.float32)
    upper_hit = (in_cells[None, :] == upper_cell[:, None]).astype(jnp.float32)
    return lower_hit * (1.0 - fraction)[:, None] + upper_hit * fraction[:, None]

def modulate(stream, scale_vec, shift_vec):
    center = stream - lax.optimization_barrier(jnp.mean(stream, axis=-1, keepdims=True))
    variance = lax.optimization_barrier(jnp.mean(center * center, axis=-1, keepdims=True))
    return center * lax.rsqrt(variance + norm_floor) * (1.0 + scale_vec) + shift_vec

def hidden_neuron_slice(vectors):
    return vectors * lax.rsqrt(lax.optimization_barrier(jnp.sum(vectors * vectors, axis=-1, keepdims=True)) + 1.0)

def group_sum(left_rows, weight, groups):
    part_width = left_rows.shape[1] // groups
    running = jnp.zeros((left_rows.shape[0], weight.shape[1]), jnp.float32)
    for group_id in range(groups):
        partial_value = jnp.dot(left_rows[:, group_id * part_width:(group_id + 1) * part_width], weight[group_id * part_width:(group_id + 1) * part_width], preferred_element_type=jnp.float32)
        rounded = lax.optimization_barrier(partial_value.astype(jnp.bfloat16))
        running = running + rounded.astype(jnp.float32)
    return running

def attend_image(operands):
    probe_token_slab, keys_all, values_all = operands
    scores = jnp.einsum('thd,shd->hts', probe_token_slab.astype(jnp.float32), keys_all.astype(jnp.float32), precision=highest)
    row_max = lax.optimization_barrier(jnp.max(scores, axis=-1, keepdims=True))
    shifted = jnp.exp(scores - row_max)
    weights_bf = (shifted / lax.optimization_barrier(jnp.sum(shifted, axis=-1, keepdims=True))).astype(jnp.bfloat16)
    attended = jnp.einsum('hts,shd->thd', weights_bf.astype(jnp.float32), values_all.astype(jnp.float32), precision=highest)
    return attended.astype(jnp.bfloat16)

def reference(sampled_earlier_tokens, quantizer_vectors, summed_latent_canvas, latent_lift_matrix, location_tier_offset, adaptive_norm_factors, logit_sharpness, probe_match_content_matrix, mixing_projection_matrix, widening_projection_matrix, narrowing_projection_matrix, cached_lower_grid_lookups, cached_lower_grid_payloads, final_norm_factors, vocabulary_logit_matrix):
    vocab_ids = jnp.arange(VOCAB, dtype=jnp.int32)

    def embed_image(token_ids):
        onehot = (token_ids[:, None] == vocab_ids[None, :]).astype(jnp.float32)
        return jnp.dot(onehot, quantizer_vectors, precision=highest, preferred_element_type=jnp.float32)
    embedded = lax.map(embed_image, sampled_earlier_tokens).reshape(IMAGES, PREV, PREV, CVAE)
    up_matrix = interp_matrix(SIDE, PREV)
    lifted = jnp.einsum('ai,nijc->najc', up_matrix, embedded, precision=highest)
    lifted = jnp.einsum('bj,najc->nabc', up_matrix, lifted, precision=highest)
    canvas = summed_latent_canvas + lifted.reshape(IMAGES, TOK, CVAE)
    stream = jnp.einsum('ntc,cd->ntd', canvas, latent_lift_matrix, precision=highest) + location_tier_offset[None]
    for depth_ordinal in range(LAYERS):
        factors = adaptive_norm_factors[depth_ordinal]
        normed = modulate(stream, factors[:, 2][:, None], factors[:, 4][:, None]).astype(jnp.bfloat16)
        projected = jnp.dot(normed.reshape(IMAGES * TOK, D), probe_match_content_matrix[depth_ordinal].reshape(D, 3 * D), preferred_element_type=jnp.float32)
        complete_channel_group_set = projected.reshape(IMAGES, TOK, 3, HEADS, HDIM)
        probe_token_slab = (hidden_neuron_slice(complete_channel_group_set[:, :, 0]) * logit_sharpness[depth_ordinal][None, None, :, None]).astype(jnp.bfloat16)
        key_new = hidden_neuron_slice(complete_channel_group_set[:, :, 1]).astype(jnp.bfloat16)
        value_new = complete_channel_group_set[:, :, 2].astype(jnp.bfloat16)
        key_old = hidden_neuron_slice(cached_lower_grid_lookups[depth_ordinal].astype(jnp.float32).reshape(IMAGES, CACHE, HEADS, HDIM)).astype(jnp.bfloat16)
        value_old = cached_lower_grid_payloads[depth_ordinal].reshape(IMAGES, CACHE, HEADS, HDIM)
        keys_all = jnp.concatenate([key_old, key_new], axis=1)
        values_all = jnp.concatenate([value_old, value_new], axis=1)
        attended = lax.map(attend_image, (probe_token_slab, keys_all, values_all))
        mixed_rows = group_sum(attended.reshape(IMAGES * TOK, D), mixing_projection_matrix[depth_ordinal], N_TENSOR)
        stream = stream + factors[:, 0][:, None] * mixed_rows.reshape(IMAGES, TOK, D)
        normed = modulate(stream, factors[:, 3][:, None], factors[:, 5][:, None]).astype(jnp.bfloat16)
        hidden = jax.nn.gelu(jnp.dot(normed.reshape(IMAGES * TOK, D), widening_projection_matrix[depth_ordinal], preferred_element_type=jnp.float32), approximate=True).astype(jnp.bfloat16)
        mixed_rows = group_sum(hidden, narrowing_projection_matrix[depth_ordinal], N_TENSOR)
        stream = stream + factors[:, 1][:, None] * mixed_rows.reshape(IMAGES, TOK, D)
    normed = modulate(stream, final_norm_factors[:, 0][:, None], final_norm_factors[:, 1][:, None]).astype(jnp.bfloat16)
    logits = jnp.dot(normed.reshape(IMAGES * TOK, D), vocabulary_logit_matrix, preferred_element_type=jnp.float32).astype(jnp.bfloat16)
    return (logits.reshape(IMAGES, TOK, VOCAB), canvas)
```

```python
import functools

import jax
import jax.numpy as jnp
from jax import lax
from jax.experimental import pallas as pl
from jax.experimental.pallas import tpu as pltpu
from jax.sharding import PartitionSpec as P

SIDE = 16
PREV = 13


norm_floor = 0.1
highest = lax.Precision.HIGHEST


def interp_matrix(grid_side, prev_side):
    out_cells = jnp.arange(grid_side, dtype=jnp.int32)
    numerator = jnp.maximum((2 * out_cells + 1) * prev_side - grid_side, 0)
    lower_cell = numerator // (2 * grid_side)
    fraction = (numerator % (2 * grid_side)).astype(jnp.float32) / (2.0 * grid_side)
    upper_cell = jnp.minimum(lower_cell + 1, prev_side - 1)
    in_cells = jnp.arange(prev_side, dtype=jnp.int32)
    lower_hit = (in_cells[None, :] == lower_cell[:, None]).astype(jnp.float32)
    upper_hit = (in_cells[None, :] == upper_cell[:, None]).astype(jnp.float32)
    return lower_hit * (1.0 - fraction)[:, None] + upper_hit * fraction[:, None]


def modulate(stream, scale_vec, shift_vec):
    center = stream - jnp.mean(stream, axis=-1, keepdims=True)
    variance = jnp.mean(center * center, axis=-1, keepdims=True)
    return center * lax.rsqrt(variance + norm_floor) * (1.0 + scale_vec) + shift_vec


def hidden_neuron_slice(vectors):
    return vectors * lax.rsqrt(jnp.sum(vectors * vectors, axis=-1, keepdims=True) + 1.0)


def shift_pairs(total, flip):
    return [(index, index ^ flip) for index in range(total)]


def gather_blocks(shard, dp_total):
    outer = dp_total // 2
    rows = shard.shape[0]
    me = lax.axis_index("dp")
    my_outer = me // 2
    my_inner = me % 2
    gathered = jnp.zeros((dp_total * rows, shard.shape[1]), shard.dtype)
    for hop in range(outer):
        if hop == 0:
            block = shard
        else:
            block = lax.ppermute(
                shard,
                "dp",
                [(i, ((i // 2 + hop) % outer) * 2 + i % 2) for i in range(dp_total)],
            )
        other = lax.ppermute(block, "dp", shift_pairs(dp_total, 1))
        source = ((my_outer - hop) % outer) * 2
        gathered = lax.dynamic_update_slice(gathered, block, ((source + my_inner) * rows, 0))
        gathered = lax.dynamic_update_slice(gathered, other, ((source + 1 - my_inner) * rows, 0))
    return gathered


def attend_kernel(head_total, head_size, image_ref, sharp_ref, proj_ref, key_ref, value_ref, out_ref):
    width = head_total * head_size

    def dot_t(left, right):
        return lax.dot_general(
            left, right, (((1,), (1,)), ((), ())), preferred_element_type=jnp.float32
        )

    for head in range(head_total):
        low = head * head_size
        high = low + head_size
        query = (
            hidden_neuron_slice(proj_ref[:, low:high]) * sharp_ref[0, head]
        ).astype(jnp.bfloat16)
        key_new = hidden_neuron_slice(proj_ref[:, width + low : width + high]).astype(jnp.bfloat16)
        value_new = proj_ref[:, 2 * width + low : 2 * width + high].astype(jnp.bfloat16)
        key_old = hidden_neuron_slice(key_ref[0, :, low:high].astype(jnp.float32)).astype(
            jnp.bfloat16
        )
        value_old = value_ref[0, :, low:high]
        score_old = dot_t(query, key_old)
        score_new = dot_t(query, key_new)
        row_max = jnp.maximum(
            jnp.max(score_old, axis=-1, keepdims=True), jnp.max(score_new, axis=-1, keepdims=True)
        )
        exp_old = jnp.exp(score_old - row_max)
        exp_new = jnp.exp(score_new - row_max)
        inverse = 1.0 / (
            jnp.sum(exp_old, axis=-1, keepdims=True) + jnp.sum(exp_new, axis=-1, keepdims=True)
        )
        weight_old = (exp_old * inverse).astype(jnp.bfloat16)
        weight_new = (exp_new * inverse).astype(jnp.bfloat16)
        mixed = jnp.dot(weight_old, value_old, preferred_element_type=jnp.float32) + jnp.dot(
            weight_new, value_new, preferred_element_type=jnp.float32
        )
        out_ref[:, low:high] = mixed.astype(jnp.bfloat16)


def attend(first_image, sharpness, projected, cached_keys, cached_values, tokens_image):
    head_total = sharpness.shape[1]
    _, cache_len, width = cached_keys.shape
    rows = projected.shape[0]
    images = rows // tokens_image
    flops = 4 * rows * (cache_len + tokens_image) * width
    return pl.pallas_call(
        functools.partial(attend_kernel, head_total, width // head_total),
        out_shape=jax.ShapeDtypeStruct((rows, width), jnp.bfloat16),
        grid_spec=pltpu.PrefetchScalarGridSpec(
            num_scalar_prefetch=1,
            grid=(images,),
            in_specs=[
                pl.BlockSpec(memory_space=pltpu.SMEM),
                pl.BlockSpec((tokens_image, 3 * width), lambda i, s: (i, 0)),
                pl.BlockSpec((1, cache_len, width), lambda i, s: (s[0] + i, 0, 0)),
                pl.BlockSpec((1, cache_len, width), lambda i, s: (s[0] + i, 0, 0)),
            ],
            out_specs=pl.BlockSpec((tokens_image, width), lambda i, s: (i, 0)),
        ),
        compiler_params=pltpu.CompilerParams(vmem_limit_bytes=24 * 1024 * 1024),
        cost_estimate=pl.CostEstimate(
            flops=flops * 6, bytes_accessed=rows * width * 14, transcendentals=flops // width
        ),
        name="attend",
    )(first_image, sharpness, projected, cached_keys, cached_values)


def local(
    dp_total,
    tensor_total,
    sampled_earlier_tokens,
    quantizer_vectors,
    summed_latent_canvas,
    latent_lift_matrix,
    location_tier_offset,
    adaptive_norm_factors,
    logit_sharpness,
    probe_match_content_matrix,
    mixing_projection_matrix,
    widening_projection_matrix,
    narrowing_projection_matrix,
    cached_lower_grid_lookups,
    cached_lower_grid_payloads,
    final_norm_factors,
    vocabulary_logit_matrix,
):
    images = sampled_earlier_tokens.shape[0]
    tokens_image = location_tier_offset.shape[0]
    channels = quantizer_vectors.shape[1]
    own_images = images // tensor_total
    own_rows = own_images * tokens_image
    assert tensor_total == 4 and images % tensor_total == 0 and dp_total % 2 == 0
    me = lax.axis_index("tensor")
    near = functools.partial(
        lax.ppermute, axis_name="tensor", perm=shift_pairs(tensor_total, 1)
    )
    far = functools.partial(lax.ppermute, axis_name="tensor", perm=shift_pairs(tensor_total, 2))

    def first_image(piece):
        return (me ^ piece) * own_images

    def own(array):
        return lax.dynamic_slice_in_dim(array, first_image(0), own_images, axis=0)

    qkv_full = gather_blocks(
        probe_match_content_matrix[0].reshape(probe_match_content_matrix.shape[1], -1), dp_total
    )
    out_full = gather_blocks(mixing_projection_matrix[0].T, dp_total)
    up_full = gather_blocks(widening_projection_matrix[0], dp_total)
    down_full = gather_blocks(narrowing_projection_matrix[0].T, dp_total)

    def times(left, right):
        return jnp.dot(left, right, preferred_element_type=jnp.float32)

    def times_t(left, right):
        return lax.dot_general(
            left, right, (((1,), (1,)), ((), ())), preferred_element_type=jnp.float32
        )

    def spread(own_piece):
        by_near = near(own_piece)
        by_far = far(own_piece)
        return [own_piece, by_near, by_far, near(by_far)]

    def collect(make_piece):
        across = near(make_piece(3).astype(jnp.bfloat16))
        far_sum = make_piece(2) + across.astype(jnp.float32)
        from_far = far(far_sum.astype(jnp.bfloat16))
        from_near = near(make_piece(1).astype(jnp.bfloat16))
        return make_piece(0) + from_near.astype(jnp.float32) + from_far.astype(jnp.float32)

    vocab_ids = jnp.arange(quantizer_vectors.shape[0], dtype=jnp.int32)
    token_ids = own(sampled_earlier_tokens).reshape(-1)
    onehot = (token_ids[:, None] == vocab_ids[None, :]).astype(jnp.float32)
    embedded = jnp.dot(
        onehot, quantizer_vectors, precision=highest, preferred_element_type=jnp.float32
    ).reshape(own_images, PREV, PREV, channels)
    up_matrix = interp_matrix(SIDE, PREV)
    lifted = jnp.einsum("ai,nijc->najc", up_matrix, embedded, precision=highest)
    lifted = jnp.einsum("bj,najc->nabc", up_matrix, lifted, precision=highest)
    own_canvas = own(summed_latent_canvas) + lifted.reshape(own_images, tokens_image, channels)
    stream = (
        jnp.einsum("ntc,cd->ntd", own_canvas, latent_lift_matrix, precision=highest)
        + location_tier_offset[None]
    )
    factors = own(adaptive_norm_factors[0])[:, :, None, :]
    head_factors = own(final_norm_factors)[:, :, None, :]

    def normed_rows(values, scale_vec, shift_vec):
        return modulate(values, scale_vec, shift_vec).astype(jnp.bfloat16).reshape(own_rows, -1)

    pieces = spread(normed_rows(stream, factors[:, 2], factors[:, 4]))

    def attention_piece(piece):
        projected = times(pieces[piece], qkv_full)
        attended = attend(
            first_image(piece).reshape(1),
            logit_sharpness,
            projected,
            cached_lower_grid_lookups[0],
            cached_lower_grid_payloads[0],
            tokens_image,
        )
        return times_t(attended, out_full)

    mixed = collect(attention_piece).reshape(stream.shape)
    stream = stream + factors[:, 0] * mixed
    unit_pieces = spread(normed_rows(stream, factors[:, 3], factors[:, 5]))

    def unit_piece(piece):
        lifted_units = times(unit_pieces[piece], up_full)
        hidden = jax.nn.gelu(lifted_units, approximate=True).astype(jnp.bfloat16)
        return times_t(hidden, down_full)

    mixed = collect(unit_piece).reshape(stream.shape)
    stream = stream + factors[:, 1] * mixed
    last_pieces = spread(normed_rows(stream, head_factors[:, 0], head_factors[:, 1]))
    canvas_pieces = spread(own_canvas)
    canvas = jnp.zeros(summed_latent_canvas.shape, jnp.float32)
    logits = jnp.zeros((images * tokens_image, vocabulary_logit_matrix.shape[1]), jnp.bfloat16)
    for piece in range(tensor_total):
        canvas = lax.dynamic_update_slice_in_dim(
            canvas, canvas_pieces[piece], first_image(piece), axis=0
        )
        logits = lax.dynamic_update_slice_in_dim(
            logits,
            times(last_pieces[piece], vocabulary_logit_matrix).astype(jnp.bfloat16),
            first_image(piece) * tokens_image,
            axis=0,
        )
    return (logits.reshape(images, tokens_image, -1), canvas)


def solution(mesh):
    placed = (
        P("dp", None),
        P(),
        P("dp", None, None),
        P(),
        P(),
        P(None, "dp", None, None),
        P(None, "tensor"),
        P(None, "dp", None, "tensor"),
        P(None, "tensor", "dp"),
        P(None, "dp", "tensor"),
        P(None, "tensor", "dp"),
        P(None, "dp", None, "tensor"),
        P(None, "dp", None, "tensor"),
        P("dp", None, None),
        P(None, "tensor"),
    )
    return jax.shard_map(
        functools.partial(local, mesh.shape["dp"], mesh.shape["tensor"]),
        mesh=mesh,
        in_specs=placed,
        out_specs=(P("dp", None, "tensor"), P("dp", None, None)),
        check_vma=False,
    )
```

```python
import functools

import jax
import jax.numpy as jnp
from jax import lax
from jax.experimental import pallas as pl
from jax.experimental.pallas import tpu as pltpu
from jax.sharding import PartitionSpec as P

SIDE = 16
PREV = 13


norm_floor = 0.1
highest = lax.Precision.HIGHEST


def interp_matrix(grid_side, prev_side):
    out_cells = jnp.arange(grid_side, dtype=jnp.int32)
    numerator = jnp.maximum((2 * out_cells + 1) * prev_side - grid_side, 0)
    lower_cell = numerator // (2 * grid_side)
    fraction = (numerator % (2 * grid_side)).astype(jnp.float32) / (2.0 * grid_side)
    upper_cell = jnp.minimum(lower_cell + 1, prev_side - 1)
    in_cells = jnp.arange(prev_side, dtype=jnp.int32)
    lower_hit = (in_cells[None, :] == lower_cell[:, None]).astype(jnp.float32)
    upper_hit = (in_cells[None, :] == upper_cell[:, None]).astype(jnp.float32)
    return lower_hit * (1.0 - fraction)[:, None] + upper_hit * fraction[:, None]


def modulate(stream, scale_vec, shift_vec):
    center = stream - jnp.mean(stream, axis=-1, keepdims=True)
    variance = jnp.mean(center * center, axis=-1, keepdims=True)
    return center * lax.rsqrt(variance + norm_floor) * (1.0 + scale_vec) + shift_vec


def hidden_neuron_slice(vectors):
    return vectors * lax.rsqrt(jnp.sum(vectors * vectors, axis=-1, keepdims=True) + 1.0)


def shift_pairs(total, flip):
    return [(index, index ^ flip) for index in range(total)]


def gather_blocks(shard, dp_total):
    outer = dp_total // 2
    upper = lax.axis_index("dp") % 2 == 1
    blocks = []
    for hop in range(outer):
        block = shard
        if hop > 0:
            block = lax.ppermute(
                shard,
                "dp",
                [(i, ((i // 2 - hop) % outer) * 2 + i % 2) for i in range(dp_total)],
            )
        other = lax.ppermute(block, "dp", shift_pairs(dp_total, 1))
        blocks.append(
            jnp.concatenate(
                [jnp.where(upper, other, block), jnp.where(upper, block, other)], axis=0
            )
        )
    return blocks


def attend_kernel(head_total, head_size, image_ref, sharp_ref, proj_ref, key_ref, value_ref, out_ref):
    width = head_total * head_size

    def dot_t(left, right):
        return lax.dot_general(
            left, right, (((1,), (1,)), ((), ())), preferred_element_type=jnp.float32
        )

    for head in range(head_total):
        low = head * head_size
        high = low + head_size
        query = (
            hidden_neuron_slice(proj_ref[:, low:high]) * sharp_ref[0, head]
        ).astype(jnp.bfloat16)
        key_new = hidden_neuron_slice(proj_ref[:, width + low : width + high]).astype(jnp.bfloat16)
        value_new = proj_ref[:, 2 * width + low : 2 * width + high].astype(jnp.bfloat16)
        key_old = hidden_neuron_slice(key_ref[0, :, low:high].astype(jnp.float32)).astype(
            jnp.bfloat16
        )
        value_old = value_ref[0, :, low:high]
        score_old = dot_t(query, key_old)
        score_new = dot_t(query, key_new)
        row_max = jnp.maximum(
            jnp.max(score_old, axis=-1, keepdims=True), jnp.max(score_new, axis=-1, keepdims=True)
        )
        exp_old = jnp.exp(score_old - row_max)
        exp_new = jnp.exp(score_new - row_max)
        inverse = 1.0 / (
            jnp.sum(exp_old, axis=-1, keepdims=True) + jnp.sum(exp_new, axis=-1, keepdims=True)
        )
        weight_old = (exp_old * inverse).astype(jnp.bfloat16)
        weight_new = (exp_new * inverse).astype(jnp.bfloat16)
        mixed = jnp.dot(weight_old, value_old, preferred_element_type=jnp.float32) + jnp.dot(
            weight_new, value_new, preferred_element_type=jnp.float32
        )
        out_ref[:, low:high] = mixed.astype(jnp.bfloat16)


def attend(first_image, sharpness, projected, cached_keys, cached_values, tokens_image):
    head_total = sharpness.shape[1]
    _, cache_len, width = cached_keys.shape
    rows = projected.shape[0]
    images = rows // tokens_image
    flops = 4 * rows * (cache_len + tokens_image) * width
    return pl.pallas_call(
        functools.partial(attend_kernel, head_total, width // head_total),
        out_shape=jax.ShapeDtypeStruct((rows, width), jnp.bfloat16),
        grid_spec=pltpu.PrefetchScalarGridSpec(
            num_scalar_prefetch=1,
            grid=(images,),
            in_specs=[
                pl.BlockSpec(memory_space=pltpu.SMEM),
                pl.BlockSpec((tokens_image, 3 * width), lambda i, s: (i, 0)),
                pl.BlockSpec((1, cache_len, width), lambda i, s: (s[0] + i, 0, 0)),
                pl.BlockSpec((1, cache_len, width), lambda i, s: (s[0] + i, 0, 0)),
            ],
            out_specs=pl.BlockSpec((tokens_image, width), lambda i, s: (i, 0)),
        ),
        compiler_params=pltpu.CompilerParams(vmem_limit_bytes=24 * 1024 * 1024),
        cost_estimate=pl.CostEstimate(
            flops=flops * 6, bytes_accessed=rows * width * 14, transcendentals=flops // width
        ),
        name="attend",
    )(first_image, sharpness, projected, cached_keys, cached_values)


def local(
    dp_total,
    tensor_total,
    sampled_earlier_tokens,
    quantizer_vectors,
    summed_latent_canvas,
    latent_lift_matrix,
    location_tier_offset,
    adaptive_norm_factors,
    logit_sharpness,
    probe_match_content_matrix,
    mixing_projection_matrix,
    widening_projection_matrix,
    narrowing_projection_matrix,
    cached_lower_grid_lookups,
    cached_lower_grid_payloads,
    final_norm_factors,
    vocabulary_logit_matrix,
):
    images = sampled_earlier_tokens.shape[0]
    tokens_image = location_tier_offset.shape[0]
    channels = quantizer_vectors.shape[1]
    own_images = images // tensor_total
    own_rows = own_images * tokens_image
    assert tensor_total == 4 and images % tensor_total == 0 and dp_total % 2 == 0
    me = lax.axis_index("tensor")
    near = functools.partial(
        lax.ppermute, axis_name="tensor", perm=shift_pairs(tensor_total, 1)
    )
    far = functools.partial(lax.ppermute, axis_name="tensor", perm=shift_pairs(tensor_total, 2))

    def first_image(piece):
        return (me ^ piece) * own_images

    def own(array):
        return lax.dynamic_slice_in_dim(array, first_image(0), own_images, axis=0)

    def gather(shard):
        return gather_blocks(shard, dp_total)

    qkv_full = jnp.concatenate(
        gather(probe_match_content_matrix[0].reshape(probe_match_content_matrix.shape[1], -1))
    )
    out_full = jnp.concatenate(gather(mixing_projection_matrix[0].T))
    up_full = jnp.concatenate(gather(widening_projection_matrix[0]))
    down_blocks = gather(narrowing_projection_matrix[0].T)
    down_parts = [jnp.concatenate(down_blocks[:-1]), down_blocks[-1]]

    width = latent_lift_matrix.shape[1]
    my_column = lax.axis_index("dp") // 2 * (width // (dp_total // 2))

    def rotate(array, start):
        doubled = jnp.concatenate([array, array], axis=-1)
        return lax.dynamic_slice_in_dim(doubled, start, width, axis=array.ndim - 1)

    def times(left, right):
        return jnp.dot(left, right, preferred_element_type=jnp.float32)

    def times_t(left, right):
        return lax.dot_general(
            left, right, (((1,), (1,)), ((), ())), preferred_element_type=jnp.float32
        )

    def spread(own_piece):
        by_far = far(own_piece)
        by_near = near(own_piece)
        return [own_piece, by_near, by_far, near(by_far)]

    def collect(make_piece):
        across = near(make_piece(3).astype(jnp.bfloat16))
        far_sum = make_piece(2) + across.astype(jnp.float32)
        from_far = far(far_sum.astype(jnp.bfloat16))
        from_near = near(make_piece(1).astype(jnp.bfloat16))
        return make_piece(0) + from_near.astype(jnp.float32) + from_far.astype(jnp.float32)

    vocab_ids = jnp.arange(quantizer_vectors.shape[0], dtype=jnp.int32)
    token_ids = own(sampled_earlier_tokens).reshape(-1)
    onehot = (token_ids[:, None] == vocab_ids[None, :]).astype(jnp.float32)
    embedded = jnp.dot(
        onehot, quantizer_vectors, precision=highest, preferred_element_type=jnp.float32
    ).reshape(own_images, PREV, PREV, channels)
    up_matrix = interp_matrix(SIDE, PREV)
    lifted = jnp.einsum("ai,nijc->najc", up_matrix, embedded, precision=highest)
    lifted = jnp.einsum("bj,najc->nabc", up_matrix, lifted, precision=highest)
    own_canvas = own(summed_latent_canvas) + lifted.reshape(own_images, tokens_image, channels)
    stream = (
        jnp.einsum("ntc,cd->ntd", own_canvas, latent_lift_matrix, precision=highest)
        + location_tier_offset[None]
    )
    stream = rotate(stream, my_column)
    factors = rotate(own(adaptive_norm_factors[0]), my_column)[:, :, None, :]
    head_factors = rotate(own(final_norm_factors), my_column)[:, :, None, :]

    def normed_rows(values, scale_vec, shift_vec):
        return modulate(values, scale_vec, shift_vec).astype(jnp.bfloat16).reshape(own_rows, -1)

    pieces = spread(normed_rows(stream, factors[:, 2], factors[:, 4]))

    def attention_piece(piece):
        projected = times(pieces[piece], qkv_full)
        attended = attend(
            first_image(piece).reshape(1),
            logit_sharpness,
            projected,
            cached_lower_grid_lookups[0],
            cached_lower_grid_payloads[0],
            tokens_image,
        )
        return times_t(attended, out_full)

    mixed = collect(attention_piece).reshape(stream.shape)
    stream = stream + factors[:, 0] * mixed
    unit_pieces = spread(normed_rows(stream, factors[:, 3], factors[:, 5]))

    hidden = []
    for piece in range(tensor_total):
        lifted_units = times(unit_pieces[piece], up_full)
        hidden.append(jax.nn.gelu(lifted_units, approximate=True).astype(jnp.bfloat16))
    mixed = jnp.concatenate(
        [collect(lambda piece: times_t(hidden[piece], part)) for part in down_parts], axis=1
    ).reshape(stream.shape)
    stream = stream + factors[:, 1] * mixed
    last_own = normed_rows(stream, head_factors[:, 0], head_factors[:, 1])
    last_pieces = spread(rotate(last_own, (width - my_column) % width))
    canvas_pieces = spread(own_canvas)
    canvas = jnp.zeros(summed_latent_canvas.shape, jnp.float32)
    logits = jnp.zeros((images * tokens_image, vocabulary_logit_matrix.shape[1]), jnp.bfloat16)
    for piece in range(tensor_total):
        canvas = lax.dynamic_update_slice_in_dim(
            canvas, canvas_pieces[piece], first_image(piece), axis=0
        )
        logits = lax.dynamic_update_slice_in_dim(
            logits,
            times(last_pieces[piece], vocabulary_logit_matrix).astype(jnp.bfloat16),
            first_image(piece) * tokens_image,
            axis=0,
        )
    return (logits.reshape(images, tokens_image, -1), canvas)


def solution(mesh):
    placed = (
        P("dp", None),
        P(),
        P("dp", None, None),
        P(),
        P(),
        P(None, "dp", None, None),
        P(None, "tensor"),
        P(None, "dp", None, "tensor"),
        P(None, "tensor", "dp"),
        P(None, "dp", "tensor"),
        P(None, "tensor", "dp"),
        P(None, "dp", None, "tensor"),
        P(None, "dp", None, "tensor"),
        P("dp", None, None),
        P(None, "tensor"),
    )
    return jax.shard_map(
        functools.partial(local, mesh.shape["dp"], mesh.shape["tensor"]),
        mesh=mesh,
        in_specs=placed,
        out_specs=(P("dp", None, "tensor"), P("dp", None, None)),
        check_vma=False,
    )
```

```python
import functools

import jax
import jax.numpy as jnp
from jax import lax
from jax.experimental import pallas as pl
from jax.experimental.pallas import tpu as pltpu
from jax.sharding import PartitionSpec as P

SIDE = 16
PREV = 13


norm_floor = 0.1
highest = lax.Precision.HIGHEST


def interp_matrix(grid_side, prev_side):
    out_cells = jnp.arange(grid_side, dtype=jnp.int32)
    numerator = jnp.maximum((2 * out_cells + 1) * prev_side - grid_side, 0)
    lower_cell = numerator // (2 * grid_side)
    fraction = (numerator % (2 * grid_side)).astype(jnp.float32) / (2.0 * grid_side)
    upper_cell = jnp.minimum(lower_cell + 1, prev_side - 1)
    in_cells = jnp.arange(prev_side, dtype=jnp.int32)
    lower_hit = (in_cells[None, :] == lower_cell[:, None]).astype(jnp.float32)
    upper_hit = (in_cells[None, :] == upper_cell[:, None]).astype(jnp.float32)
    return lower_hit * (1.0 - fraction)[:, None] + upper_hit * fraction[:, None]


def modulate(stream, scale_vec, shift_vec):
    center = stream - jnp.mean(stream, axis=-1, keepdims=True)
    variance = jnp.mean(center * center, axis=-1, keepdims=True)
    return center * lax.rsqrt(variance + norm_floor) * (1.0 + scale_vec) + shift_vec


def hidden_neuron_slice(vectors):
    return vectors * lax.rsqrt(jnp.sum(vectors * vectors, axis=-1, keepdims=True) + 1.0)


def shift_pairs(total, flip):
    return [(index, index ^ flip) for index in range(total)]


def hop_lists(outer):
    own_hops = sorted({1, outer - 1} - {0}) if outer > 1 else []
    relays = []
    for depth in range(2, outer // 2 + 1):
        relays += sorted({depth, outer - depth} - set(own_hops + relays))
    return own_hops, relays


def gather_blocks(shard, dp_total):
    outer = dp_total // 2
    upper = lax.axis_index("dp") % 2 == 1

    def from_next(block, step):
        perm = [(i, ((i // 2 - step) % outer) * 2 + i % 2) for i in range(dp_total)]
        return lax.ppermute(block, "dp", perm)

    own_hops, relays = hop_lists(outer)
    held = {0: shard}
    for hop in own_hops:
        held[hop] = from_next(shard, hop)
    for hop in relays:
        if hop <= outer // 2:
            held[hop] = from_next(held[hop - 1], 1)
        else:
            held[hop] = from_next(held[hop + 1], outer - 1)
    blocks = []
    for hop in range(outer):
        other = lax.ppermute(held[hop], "dp", shift_pairs(dp_total, 1))
        blocks.append(
            jnp.concatenate(
                [jnp.where(upper, other, held[hop]), jnp.where(upper, held[hop], other)], axis=0
            )
        )
    return blocks


def attend_kernel(head_total, head_size, image_ref, sharp_ref, proj_ref, key_ref, value_ref, out_ref):
    width = head_total * head_size

    def dot_t(left, right):
        return lax.dot_general(
            left, right, (((1,), (1,)), ((), ())), preferred_element_type=jnp.float32
        )

    for head in range(head_total):
        low = head * head_size
        high = low + head_size
        query = (
            hidden_neuron_slice(proj_ref[:, low:high]) * sharp_ref[0, head]
        ).astype(jnp.bfloat16)
        key_new = hidden_neuron_slice(proj_ref[:, width + low : width + high]).astype(jnp.bfloat16)
        value_new = proj_ref[:, 2 * width + low : 2 * width + high].astype(jnp.bfloat16)
        key_old = hidden_neuron_slice(key_ref[0, :, low:high].astype(jnp.float32)).astype(
            jnp.bfloat16
        )
        value_old = value_ref[0, :, low:high]
        score_old = dot_t(query, key_old)
        score_new = dot_t(query, key_new)
        row_max = jnp.maximum(
            jnp.max(score_old, axis=-1, keepdims=True), jnp.max(score_new, axis=-1, keepdims=True)
        )
        exp_old = jnp.exp(score_old - row_max)
        exp_new = jnp.exp(score_new - row_max)
        inverse = 1.0 / (
            jnp.sum(exp_old, axis=-1, keepdims=True) + jnp.sum(exp_new, axis=-1, keepdims=True)
        )
        weight_old = (exp_old * inverse).astype(jnp.bfloat16)
        weight_new = (exp_new * inverse).astype(jnp.bfloat16)
        mixed = jnp.dot(weight_old, value_old, preferred_element_type=jnp.float32) + jnp.dot(
            weight_new, value_new, preferred_element_type=jnp.float32
        )
        out_ref[:, low:high] = mixed.astype(jnp.bfloat16)


def attend(first_image, sharpness, projected, cached_keys, cached_values, tokens_image):
    head_total = sharpness.shape[1]
    _, cache_len, width = cached_keys.shape
    rows = projected.shape[0]
    images = rows // tokens_image
    flops = 4 * rows * (cache_len + tokens_image) * width
    return pl.pallas_call(
        functools.partial(attend_kernel, head_total, width // head_total),
        out_shape=jax.ShapeDtypeStruct((rows, width), jnp.bfloat16),
        grid_spec=pltpu.PrefetchScalarGridSpec(
            num_scalar_prefetch=1,
            grid=(images,),
            in_specs=[
                pl.BlockSpec(memory_space=pltpu.SMEM),
                pl.BlockSpec((tokens_image, 3 * width), lambda i, s: (i, 0)),
                pl.BlockSpec((1, cache_len, width), lambda i, s: (s[0] + i, 0, 0)),
                pl.BlockSpec((1, cache_len, width), lambda i, s: (s[0] + i, 0, 0)),
            ],
            out_specs=pl.BlockSpec((tokens_image, width), lambda i, s: (i, 0)),
        ),
        compiler_params=pltpu.CompilerParams(vmem_limit_bytes=24 * 1024 * 1024),
        cost_estimate=pl.CostEstimate(
            flops=flops * 6, bytes_accessed=rows * width * 14, transcendentals=flops // width
        ),
        name="attend",
    )(first_image, sharpness, projected, cached_keys, cached_values)


def local(
    dp_total,
    tensor_total,
    sampled_earlier_tokens,
    quantizer_vectors,
    summed_latent_canvas,
    latent_lift_matrix,
    location_tier_offset,
    adaptive_norm_factors,
    logit_sharpness,
    probe_match_content_matrix,
    mixing_projection_matrix,
    widening_projection_matrix,
    narrowing_projection_matrix,
    cached_lower_grid_lookups,
    cached_lower_grid_payloads,
    final_norm_factors,
    vocabulary_logit_matrix,
):
    images = sampled_earlier_tokens.shape[0]
    tokens_image = location_tier_offset.shape[0]
    channels = quantizer_vectors.shape[1]
    own_images = images // tensor_total
    own_rows = own_images * tokens_image
    assert tensor_total == 4 and images % tensor_total == 0 and dp_total % 2 == 0
    me = lax.axis_index("tensor")
    near = functools.partial(
        lax.ppermute, axis_name="tensor", perm=shift_pairs(tensor_total, 1)
    )
    far = functools.partial(lax.ppermute, axis_name="tensor", perm=shift_pairs(tensor_total, 2))

    def first_image(piece):
        return (me ^ piece) * own_images

    def own(array):
        return lax.dynamic_slice_in_dim(array, first_image(0), own_images, axis=0)

    def gather(shard):
        return gather_blocks(shard, dp_total)

    qkv_full = jnp.concatenate(
        gather(probe_match_content_matrix[0].reshape(probe_match_content_matrix.shape[1], -1))
    )
    out_full = jnp.concatenate(gather(mixing_projection_matrix[0].T))
    up_full = jnp.concatenate(gather(widening_projection_matrix[0]))
    down_blocks = gather(narrowing_projection_matrix[0].T)
    last_hop = sum(hop_lists(dp_total // 2), [0])[-1]
    down_parts = [
        jnp.concatenate(down_blocks[:last_hop] + down_blocks[last_hop + 1 :]),
        down_blocks[last_hop],
    ]
    last_column = last_hop * down_blocks[0].shape[0]

    width = latent_lift_matrix.shape[1]
    my_column = lax.axis_index("dp") // 2 * (width // (dp_total // 2))

    def rotate(array, start):
        doubled = jnp.concatenate([array, array], axis=-1)
        return lax.dynamic_slice_in_dim(doubled, start, width, axis=array.ndim - 1)

    def times(left, right):
        return jnp.dot(left, right, preferred_element_type=jnp.float32)

    def times_t(left, right):
        return lax.dot_general(
            left, right, (((1,), (1,)), ((), ())), preferred_element_type=jnp.float32
        )

    def spread(own_piece):
        by_far = far(own_piece)
        by_near = near(own_piece)
        return [own_piece, by_near, by_far, near(by_far)]

    def collect(make_piece):
        across = near(make_piece(3).astype(jnp.bfloat16))
        far_sum = make_piece(2) + across.astype(jnp.float32)
        from_far = far(far_sum.astype(jnp.bfloat16))
        from_near = near(make_piece(1).astype(jnp.bfloat16))
        return make_piece(0) + from_near.astype(jnp.float32) + from_far.astype(jnp.float32)

    vocab_ids = jnp.arange(quantizer_vectors.shape[0], dtype=jnp.int32)
    token_ids = own(sampled_earlier_tokens).reshape(-1)
    onehot = (token_ids[:, None] == vocab_ids[None, :]).astype(jnp.float32)
    embedded = jnp.dot(
        onehot, quantizer_vectors, precision=highest, preferred_element_type=jnp.float32
    ).reshape(own_images, PREV, PREV, channels)
    up_matrix = interp_matrix(SIDE, PREV)
    lifted = jnp.einsum("ai,nijc->najc", up_matrix, embedded, precision=highest)
    lifted = jnp.einsum("bj,najc->nabc", up_matrix, lifted, precision=highest)
    own_canvas = own(summed_latent_canvas) + lifted.reshape(own_images, tokens_image, channels)
    stream = (
        jnp.einsum("ntc,cd->ntd", own_canvas, latent_lift_matrix, precision=highest)
        + location_tier_offset[None]
    )
    stream = rotate(stream, my_column)
    factors = rotate(own(adaptive_norm_factors[0]), my_column)[:, :, None, :]
    head_factors = rotate(own(final_norm_factors), my_column)[:, :, None, :]

    def normed_rows(values, scale_vec, shift_vec):
        return modulate(values, scale_vec, shift_vec).astype(jnp.bfloat16).reshape(own_rows, -1)

    pieces = spread(normed_rows(stream, factors[:, 2], factors[:, 4]))

    def attention_piece(piece):
        projected = times(pieces[piece], qkv_full)
        attended = attend(
            first_image(piece).reshape(1),
            logit_sharpness,
            projected,
            cached_lower_grid_lookups[0],
            cached_lower_grid_payloads[0],
            tokens_image,
        )
        return times_t(attended, out_full)

    mixed = collect(attention_piece).reshape(stream.shape)
    stream = stream + factors[:, 0] * mixed
    unit_pieces = spread(normed_rows(stream, factors[:, 3], factors[:, 5]))

    hidden = []
    for piece in range(tensor_total):
        lifted_units = times(unit_pieces[piece], up_full)
        hidden.append(jax.nn.gelu(lifted_units, approximate=True).astype(jnp.bfloat16))
    most, last = [collect(lambda piece: times_t(hidden[piece], part)) for part in down_parts]
    mixed = jnp.concatenate(
        [most[:, :last_column], last, most[:, last_column:]], axis=1
    ).reshape(stream.shape)
    stream = stream + factors[:, 1] * mixed
    last_own = normed_rows(stream, head_factors[:, 0], head_factors[:, 1])
    last_pieces = spread(rotate(last_own, (width - my_column) % width))
    canvas_pieces = spread(own_canvas)
    canvas = jnp.zeros(summed_latent_canvas.shape, jnp.float32)
    logits = jnp.zeros((images * tokens_image, vocabulary_logit_matrix.shape[1]), jnp.bfloat16)
    for piece in range(tensor_total):
        canvas = lax.dynamic_update_slice_in_dim(
            canvas, canvas_pieces[piece], first_image(piece), axis=0
        )
        logits = lax.dynamic_update_slice_in_dim(
            logits,
            times(last_pieces[piece], vocabulary_logit_matrix).astype(jnp.bfloat16),
            first_image(piece) * tokens_image,
            axis=0,
        )
    return (logits.reshape(images, tokens_image, -1), canvas)


def solution(mesh):
    placed = (
        P("dp", None),
        P(),
        P("dp", None, None),
        P(),
        P(),
        P(None, "dp", None, None),
        P(None, "tensor"),
        P(None, "dp", None, "tensor"),
        P(None, "tensor", "dp"),
        P(None, "dp", "tensor"),
        P(None, "tensor", "dp"),
        P(None, "dp", None, "tensor"),
        P(None, "dp", None, "tensor"),
        P("dp", None, None),
        P(None, "tensor"),
    )
    return jax.shard_map(
        functools.partial(local, mesh.shape["dp"], mesh.shape["tensor"]),
        mesh=mesh,
        in_specs=placed,
        out_specs=(P("dp", None, "tensor"), P("dp", None, None)),
        check_vma=False,
    )
```
